32 devices in a mesh: ens: 4 (over y, x), zero: 2 (over core), cols: 4 (over z).
Axes of the slice: x: 2, y: 2, z: 4, core: 2. Of those that a mesh axis runs over, the one named last changes fastest.
Arguments:
- one_gate: float32 [8192, 8192], P(('ens', 'zero'), 'cols'), parts along dimension 0, may hold values from -0.1875 to 0.1875
- other_gate: float32 [8192, 8192], P(('ens', 'zero'), 'cols'), parts along dimension 0, may hold values from -0.125 to 0.125
- one_up: float32 [8192, 8192], P(('ens', 'zero'), 'cols'), parts along dimension 0, may hold values from -0.1875 to 0.1875
- other_up: float32 [8192, 8192], P(('ens', 'zero'), 'cols'), parts along dimension 0, may hold values from -0.125 to 0.125
- mix_share: float32 [8192], P(('ens', 'zero')), parts along dimension 0, may hold values from 0.2 to 0.8
- norm_train: float32 [8192], P(('ens', 'zero', 'cols')), parts along dimension 0, may hold values from 0.25 to 1.75
- norm_step: float32 [8192], P(('ens', 'zero', 'cols')), parts along dimension 0, may hold values from -0.3 to 0.3
Outputs:
- serve_gate: bfloat16 [8192, 8192], P('ens', 'cols'), parts along dimension 0
- serve_up: bfloat16 [8192, 8192], P('ens', 'cols'), parts along dimension 0
- factor_gate: float32 [32768], P(('ens', 'cols')), parts along dimension 0
- factor_up: float32 [32768], P(('ens', 'cols')), parts along dimension 0
- serve_norm: bfloat16 [8192], P('ens'), parts along dimension 0
The draws below stay inside these ranges and needn't reach their ends.
There are 4 independent parts, one for each index of `ens`. The reference program is written for one: setup_inputs(seed, part) draws one part's arguments, and reference() takes and returns one part's arrays. A program takes and returns all parts, laid end to end along the dimension named above; each array names one. Nothing has to cross between parts.
All inputs are finite; a program needn't handle non-finite values. Where the reference program divides by a largest or mean magnitude, that divisor is 1e-20 or more.
Results may differ from the reference program's by a relative error of at most 0.001.
Values may be sent and summed in bfloat16 or wider, within the bound.
A program may use at most 128 MiB of HBM per device.

```python
import jax
import jax.numpy as jnp

D_MODEL = 2048
D_INNER = 8192


def with_spikes(values, key, source, target, parts, factor):
    owner, partner = [(jnp.arange(values.shape[axis_at]) // (values.shape[axis_at] // parts)).reshape([-1 if axis == axis_at else 1 for axis in range(values.ndim)]) for axis_at in (source, target)]
    chosen = jax.random.permutation(key, parts)[partner]
    strong = (owner == chosen) | (owner == (partner + parts // 2) % parts)
    return jnp.where(strong, factor * values, values)


def levels(rng, extent, split, least, high):
    level = 1.0
    for axis_at, shards_of in split:
        heights = jax.random.uniform(jax.random.fold_in(jax.random.fold_in(rng, 6), axis_at), (shards_of,), jnp.float32, least / len(split), high / len(split))
        level = level * jnp.repeat(jnp.exp(heights), extent[axis_at] // shards_of).reshape((-1,) + (1,) * (len(extent) - 1 - axis_at))
    return level


def centred(stream_key, extent, deviation, bound, cuts=(), held_as=jnp.bfloat16):
    factor_of = levels(stream_key, extent, cuts, -0.22, 0.18) if cuts else 1.0
    entries = jax.random.normal(stream_key, extent, jnp.float32) * deviation * factor_of
    return jnp.minimum(jnp.maximum(entries, -bound), bound).astype(held_as)


def bell_draw_with(rng, extent, scale, limit, split, heavy, held_as=jnp.bfloat16):
    drawn = scale * jax.random.normal(rng, extent, jnp.float32)
    if split:
        drawn = drawn * levels(rng, extent, split, -0.22, 0.18)
    return jnp.clip(with_spikes(drawn, jax.random.fold_in(rng, 3), *heavy), -limit, limit).astype(held_as)


def setup_inputs(seed: int = 0, part: int = 0) -> dict:
    streams_of = jax.random.split(jax.random.key(seed), 8)
    part_splits = jax.random.split(jax.random.fold_in(streams_of[7], part), 8)
    one_gate = bell_draw_with(part_splits[0], (D_MODEL, D_INNER), D_MODEL ** -0.5, 0.1875, ((0, 2), (1, 4)), (0, 1, 4, 2.0), jnp.float32)
    other_gate = centred(part_splits[1], (D_MODEL, D_INNER), D_MODEL ** -0.5, 0.125, ((0, 2), (1, 4)), jnp.float32)
    one_up = bell_draw_with(part_splits[2], (D_MODEL, D_INNER), D_MODEL ** -0.5, 0.1875, ((0, 2), (1, 4)), (0, 1, 4, 2.0), jnp.float32)
    other_up = centred(part_splits[3], (D_MODEL, D_INNER), D_MODEL ** -0.5, 0.125, ((0, 2), (1, 4)), jnp.float32)
    mix_share = jnp.clip(0.2 + 0.6 * jax.random.uniform(part_splits[4], (D_MODEL,), jnp.float32) ** levels(part_splits[4], (D_MODEL,), ((0, 2),), -0.2, 0.2), 0.2, 0.8)
    norm_train = jnp.clip(1.0 + 0.15 * jax.random.normal(part_splits[5], (D_MODEL,), jnp.float32), 0.25, 1.75)
    norm_step = jnp.clip(jax.random.uniform(part_splits[6], (D_MODEL,), jnp.float32, -0.3, 0.3) * levels(part_splits[6], (D_MODEL,), ((0, 8),), -0.4, 0.0), -0.3, 0.3)
    return {"one_gate": one_gate, "other_gate": other_gate, "one_up": one_up, "other_up": other_up, "mix_share": mix_share, "norm_train": norm_train, "norm_step": norm_step}


def reference(one_gate, other_gate, one_up, other_up, mix_share, norm_train, norm_step):
    fresh_gate = mix_share[:, None] * one_gate + (1.0 - mix_share[:, None]) * other_gate
    fresh_up = mix_share[:, None] * one_up + (1.0 - mix_share[:, None]) * other_up
    factor_gate = jnp.sum(jnp.abs(fresh_gate), axis=0) / D_MODEL
    serve_gate = (fresh_gate / factor_gate).astype(jnp.bfloat16)
    factor_up = jnp.sum(jnp.abs(fresh_up), axis=0) / D_MODEL
    serve_up = (fresh_up / factor_up).astype(jnp.bfloat16)
    serve_norm = (norm_train + norm_step).astype(jnp.bfloat16)
    return serve_gate, serve_up, factor_gate, factor_up, serve_norm
```

```python
import functools

import jax
import jax.numpy as jnp
from jax import lax
from jax.experimental import pallas as pl
from jax.experimental.pallas import tpu as pltpu
from jax.sharding import PartitionSpec as P

MESH = pl.DeviceIdType.MESH
LANES = 128
WIDTH = 256
SLOTS = 4
FRESH = 4
LAG = 2
BLOCK = 64


def exchange(
    n, m,
    one_gate, other_gate, one_up, other_up, mix, norm_train, norm_step,
    gate, up, factor_gate, factor_up, norm,
    one_buf, other_buf, fresh, mixed, sums, norm_buf,
    read_sem, sum_send, sum_recv, data_send, data_recv, norm_send, norm_recv,
):
    me, z = lax.axis_index("zero"), lax.axis_index("cols")
    rows, cols = one_gate.shape
    width = one_buf.shape[-1]
    per = cols // width
    base = pl.multiple_of(me * rows, rows)
    block = min(BLOCK, rows)
    work = [
        (src, other, out, factor, k)
        for src, other, out, factor in (
            (one_gate, other_gate, gate, factor_gate),
            (one_up, other_up, up, factor_up),
        )
        for k in range(per)
    ]
    total = len(work)

    def reads(c):
        src, other, _, _, k = work[c]
        at, slot = pl.ds(k * width, width), c % SLOTS
        return (
            pltpu.make_async_copy(src.at[:, at], one_buf.at[slot], read_sem.at[0, slot]),
            pltpu.make_async_copy(other.at[:, at], other_buf.at[slot], read_sem.at[1, slot]),
        )

    def sum_copy(c, d):
        return pltpu.make_async_remote_copy(
            src_ref=sums.at[c, me], dst_ref=sums.at[c, me],
            send_sem=sum_send.at[c], recv_sem=sum_recv.at[c],
            device_id={"zero": lax.rem(me + d, n)}, device_id_type=MESH,
        )

    def data_copy(c, d):
        _, _, out, _, k = work[c]
        at = out.at[pl.ds(base, rows), pl.ds(k * width, width)]
        return pltpu.make_async_remote_copy(
            src_ref=at, dst_ref=at,
            send_sem=data_send.at[c], recv_sem=data_recv.at[c],
            device_id={"zero": lax.rem(me + d, n)}, device_id_type=MESH,
        )

    others = [(dz, dc) for dz in range(n) for dc in range(m) if dz or dc]

    def place(dz, dc):
        return {"zero": lax.rem(me + dz, n), "cols": lax.rem(z + dc, m)}

    def norm_copy(i):
        at = norm_buf.at[me * m + z]
        return pltpu.make_async_remote_copy(
            src_ref=at, dst_ref=at,
            send_sem=norm_send.at[i], recv_sem=norm_recv.at[i],
            device_id=place(*others[i]), device_id_type=MESH,
        )

    def blend(c):
        slot, keep = c % SLOTS, c % FRESH
        for copy in reads(c):
            copy.wait()

        def step(r, acc):
            at = pl.ds(pl.multiple_of(r * block, block), block)
            share = mixed[at, :]
            rest = 1.0 - share
            new = []
            for j in range(width // LANES):
                lanes = pl.ds(j * LANES, LANES)
                value = share * one_buf[slot, at, lanes] + rest * other_buf[slot, at, lanes]
                fresh[keep, at, lanes] = value
                new.append(acc[j] + jnp.sum(jnp.abs(value).reshape(-1, 8, LANES), axis=0))
            return tuple(new)

        zero = jnp.zeros((8, LANES), jnp.float32)
        acc = lax.fori_loop(0, rows // block, step, (zero,) * (width // LANES))
        for j in range(width // LANES):
            sums[c, me, :, pl.ds(j * LANES, LANES)] = jnp.sum(acc[j], axis=0, keepdims=True)
        if c + SLOTS < total:
            for copy in reads(c + SLOTS):
                copy.start()

    def scale(c):
        _, _, out, factor_out, k = work[c]
        keep = c % FRESH
        for d in range(1, n):
            sum_copy(c, d).wait()
        factor = sums[c, 0]
        for i in range(1, n):
            factor = factor + sums[c, i]
        factor = factor / (n * rows)
        factor_out[:, pl.ds(k * width, width)] = factor
        inverse = 1.0 / factor

        def step(r, carry):
            at = pl.multiple_of(r * block, block)
            for j in range(width // LANES):
                value = fresh[keep, pl.ds(at, block), pl.ds(j * LANES, LANES)]
                out[pl.ds(base + at, block), pl.ds(k * width + j * LANES, LANES)] = (
                    value * inverse[:, j * LANES:(j + 1) * LANES]
                ).astype(out.dtype)
            return carry

        lax.fori_loop(0, rows // block, step, 0)
        for d in range(1, n):
            data_copy(c, d).start()

    for c in range(min(SLOTS, total)):
        for copy in reads(c):
            copy.start()
    barrier = pltpu.get_barrier_semaphore()
    for dz, dc in others:
        pl.semaphore_signal(barrier, inc=1, device_id=place(dz, dc), device_id_type=MESH)
    norm_buf[me * m + z] = norm_train[...] + norm_step[...]
    for k in range(rows // LANES):
        row = mix[pl.ds(k, 1), :]
        mixed[pl.ds(k * LANES, LANES), :] = jnp.transpose(jnp.broadcast_to(row, (LANES, LANES)))
    pl.semaphore_wait(barrier, len(others))

    for c in range(total + LAG):
        if c < total:
            blend(c)
            for d in range(1, n):
                sum_copy(c, d).start()
        if c == LAG - 1:
            for i in range(len(others)):
                norm_copy(i).start()
        if c >= LAG:
            scale(c - LAG)
    for i in range(len(others)):
        norm_copy(i).wait()
    norm[...] = norm_buf[...]
    for c in range(total):
        for d in range(1, n):
            data_copy(c, d).wait()


def write(
    pieces, gate, up, factor_gate_in, factor_up_in,
    gate_out, up_out, factor_gate, factor_up, sem,
):
    depth = gate.shape[0] // pieces
    copies = [
        pltpu.make_async_copy(
            src.at[pl.ds(i * depth, depth)], dst.at[pl.ds(i * depth, depth)], sem.at[a, i]
        )
        for a, (src, dst) in enumerate(((gate, gate_out), (up, up_out)))
        for i in range(pieces)
    ]
    for copy in copies:
        copy.start()
    factor_gate[...] = factor_gate_in[...]
    factor_up[...] = factor_up_in[...]
    for copy in copies:
        copy.wait()


def local(n, m, one_gate, other_gate, one_up, other_up, mix_share, norm_train, norm_step):
    rows, cols = one_gate.shape
    (own,) = norm_train.shape
    width = min(WIDTH, cols)
    total = 2 * (cols // width)
    whole = (n * rows, cols)
    hbm = pl.BlockSpec(memory_space=pl.ANY)
    vmem = pl.BlockSpec(memory_space=pltpu.VMEM)
    dma = pltpu.SemaphoreType.DMA
    gate, up, factor_gate, factor_up, norm = pl.pallas_call(
        functools.partial(exchange, n, m),
        out_shape=(
            pltpu.VMEM(whole, jnp.bfloat16),
            pltpu.VMEM(whole, jnp.bfloat16),
            jax.ShapeDtypeStruct((1, cols), jnp.float32),
            jax.ShapeDtypeStruct((1, cols), jnp.float32),
            jax.ShapeDtypeStruct((n * m, 1, own), jnp.float32),
        ),
        in_specs=[hbm] * 4 + [vmem] * 3,
        out_specs=(vmem,) * 5,
        scratch_shapes=[
            pltpu.VMEM((SLOTS, rows, width), jnp.float32),
            pltpu.VMEM((SLOTS, rows, width), jnp.float32),
            pltpu.VMEM((FRESH, rows, width), jnp.float32),
            pltpu.VMEM((rows, LANES), jnp.float32),
            pltpu.VMEM((total, n, 1, width), jnp.float32),
            pltpu.VMEM((n * m, 1, own), jnp.float32),
            dma((2, SLOTS)),
            dma((total,)),
            dma((total,)),
            dma((total,)),
            dma((total,)),
            dma((n * m - 1,)),
            dma((n * m - 1,)),
        ],
        compiler_params=pltpu.CompilerParams(
            collective_id=0, has_side_effects=True, vmem_limit_bytes=36 * 2**20
        ),
        name="exchange",
    )(
        one_gate, other_gate, one_up, other_up,
        mix_share.reshape(-1, LANES), norm_train.reshape(1, -1), norm_step.reshape(1, -1),
    )
    pieces = 8
    serve_gate, serve_up, factor_gate, factor_up = pl.pallas_call(
        functools.partial(write, pieces),
        out_shape=(
            jax.ShapeDtypeStruct(whole, jnp.bfloat16),
            jax.ShapeDtypeStruct(whole, jnp.bfloat16),
            jax.ShapeDtypeStruct((1, cols), jnp.float32),
            jax.ShapeDtypeStruct((1, cols), jnp.float32),
        ),
        in_specs=[vmem] * 4,
        out_specs=(hbm, hbm, vmem, vmem),
        scratch_shapes=[dma((2, pieces))],
        compiler_params=pltpu.CompilerParams(vmem_limit_bytes=2**20),
        name="write",
    )(gate, up, factor_gate, factor_up)
    return (
        serve_gate, serve_up, factor_gate.reshape(-1), factor_up.reshape(-1),
        norm.reshape(-1).astype(jnp.bfloat16),
    )


def solution(mesh):
    return jax.shard_map(
        functools.partial(local, mesh.shape["zero"], mesh.shape["cols"]),
        mesh=mesh,
        in_specs=(P(("ens", "zero"), "cols"),) * 4
        + (P(("ens", "zero")), P(("ens", "zero", "cols")), P(("ens", "zero", "cols"))),
        out_specs=(P("ens", "cols"), P("ens", "cols"), P(("ens", "cols")), P(("ens", "cols")), P("ens")),
        check_vma=False,
    )
```
